32 devices in a mesh: sfc: 32 (over z, y, x, core).
Axes of the slice: x: 2, y: 2, z: 4, core: 2. Of those that a mesh axis runs over, the one named last changes fastest.
Arguments:
- tracers: float32 [2048, 3, 480], P('sfc'), may hold values from -6 to 6
- weights: float32 [2, 2048, 3, 256], P(None, 'sfc'), may hold values from -1.5 to 1.5
- departure: int32 [2048, 48], P('sfc'), may hold values from 0 to 95, as said below
- needs: int32 [32, 8, 4], P('sfc'), may hold values from 0 to 63
- counts: int32 [32, 8], P('sfc'), may hold values from 1 to 4, as said below
Outputs:
- mixed: float32 [2048, 3, 480], P('sfc')
The draws below stay inside these ranges and needn't reach their ends.
Inputs may be any that keep to these rules, and one draw needn't show every extreme that they name: `departure`: each entry is a slot of its range's source table: below 64 a local element; otherwise 64 + j * 4 + c with c below counts[r, j] of its range r. `counts`: some range uses all 4 entries of every list in every draw.
All inputs are finite; a program needn't handle non-finite values.
Results may differ from the reference program's by a relative error of at most 0.0003.
Values sent between devices are 32-bit elements; how exact they have to be, the bound alone decides.
A program may use at most 64 MiB of HBM per device.

```python
import math
import jax
import jax.numpy as jnp
from jax import lax

NODES = 16
TRACERS = 30
LEV = 3
SUBSTEPS = 2
REACH = 4
CAP = 4
ELEMS = 64
ELEMS_ALL = 2048
N_SFC = 32


def counts_table(key):
    ranks_total = ELEMS_ALL // ELEMS
    folded = jax.random.fold_in(key, 11)
    key_counts, key_band = jax.random.split(folded)
    drawn = jax.random.randint(key_counts, (ranks_total, 2 * REACH), 1, CAP + 1)
    band_start = jax.random.randint(key_band, (), 0, ranks_total)
    in_band = (jnp.arange(ranks_total) - band_start) % ranks_total < max(ranks_total // 4, 1)
    return jnp.where(in_band[:, None], CAP, drawn).astype(jnp.int32)


def draw_counts(key, part):
    return counts_table(key)


def draw_departure(key, part):
    limits_table = counts_table(key)
    folded = jax.random.fold_in(key, 23)
    key_remote, key_offset, key_column, key_local = jax.random.split(folded, 4)
    grid_shape = (ELEMS_ALL, LEV * NODES)
    owner_rank = (jnp.arange(ELEMS_ALL) // ELEMS)[:, None]
    remote = jax.random.randint(key_remote, grid_shape, 0, 10) < 3
    offset_pick = jax.random.randint(key_offset, grid_shape, 0, 2 * REACH)
    raw_bits = jax.random.randint(key_column, grid_shape, 0, 1 << 20)
    limits = limits_table[owner_rank, offset_pick]
    column = raw_bits % limits
    local_pick = jax.random.randint(key_local, grid_shape, 0, ELEMS)
    return jnp.where(remote, ELEMS + offset_pick * CAP + column, local_pick).astype(jnp.int32)


def set_ends(entries, rng, smallest, high):
    place = [jax.random.randint(jax.random.fold_in(rng, axis), (), 0, length) for axis, length in enumerate(entries.shape)]
    longest = entries.shape.index(max(entries.shape))
    next_to = place[:longest] + [(place[longest] + 1) % entries.shape[longest]] + place[longest + 1:]
    return entries.at[tuple(place)].set(smallest).at[tuple(next_to)].set(high)


def block_scale(stream_key, extent, cuts, least, top_value):
    gain = 1.0
    for position, shards_of in cuts:
        draws = jax.random.uniform(jax.random.fold_in(jax.random.fold_in(stream_key, 6), position), (shards_of,), jnp.float32, least / len(cuts), top_value / len(cuts))
        gain = gain * jnp.repeat(jnp.exp(draws), extent[position] // shards_of).reshape((-1,) + (1,) * (len(extent) - 1 - position))
    return gain


def normal_values(key, dims, spread, bound, pieces=(), held_as=jnp.bfloat16):
    values = spread * jax.random.normal(key, dims, jnp.float32)
    if pieces:
        values = values * block_scale(key, dims, pieces, -0.22, 0.18)
    return jnp.clip(values, -bound, bound).astype(held_as)


def setup_inputs(seed: int = 0) -> dict:
    seeds = jax.random.split(jax.random.key(seed), 6)
    return {
        "tracers": normal_values(seeds[0], (ELEMS_ALL, LEV, NODES * TRACERS), 1.0, 6.0, ((0, 32),), jnp.float32),
        "weights": normal_values(seeds[1], (SUBSTEPS, ELEMS_ALL, LEV, NODES * NODES), NODES ** -0.5, 1.5, ((1, 32),), jnp.float32),
        "departure": draw_departure(jax.random.fold_in(seeds[5], 71), 0),
        "needs": set_ends(jax.random.randint(seeds[3], (N_SFC, 2 * REACH, CAP), 0, ELEMS), jax.random.fold_in(seeds[3], 1), 0, ELEMS - 1).astype(jnp.int32),
        "counts": draw_counts(jax.random.fold_in(seeds[5], 71), 0),
    }


def interpolate(source_table, dep_block, weight_block):
    elements = dep_block.shape[0]
    block_rows = math.gcd(elements, 32)
    flat_rows = source_table.reshape(-1, NODES * TRACERS)
    slot_rows = dep_block.reshape(elements, LEV, NODES) * LEV + jnp.arange(LEV, dtype=jnp.int32)[None, :, None]

    def per_block(inputs):
        row_index, matrices = inputs
        gathered = flat_rows[row_index].reshape(block_rows, LEV, NODES, NODES, TRACERS)
        matrices = matrices.reshape(block_rows, LEV, NODES, NODES)
        values = jnp.einsum("elts,eltsq->eltq", matrices, gathered, precision=lax.Precision.HIGHEST)
        lowest = jnp.min(gathered, axis=3)
        highest = jnp.max(gathered, axis=3)
        return jnp.clip(values, lowest, highest).reshape(block_rows, LEV, NODES * TRACERS)

    result = lax.map(per_block, (slot_rows.reshape(elements // block_rows, block_rows, LEV, NODES),
                                 weight_block.reshape(elements // block_rows, block_rows, LEV, NODES * NODES)))
    return result.reshape(elements, LEV, NODES * TRACERS)


def reference(tracers, weights, departure, needs, counts):
    offset_order = jnp.arange(2 * REACH, dtype=jnp.int32)
    offsets = jnp.where(offset_order < REACH, offset_order - REACH, offset_order - REACH + 1)
    live_slots = jnp.arange(CAP, dtype=jnp.int32)[None, None, :] < counts[:, :, None]
    current = tracers
    for substep in range(SUBSTEPS):
        def per_range(owner_rank):
            own_rows = lax.dynamic_slice_in_dim(current, owner_rank * ELEMS, ELEMS, 0)
            owners = (owner_rank + offsets) % N_SFC
            row_index = (owners[:, None] * ELEMS + needs[owner_rank]).astype(jnp.int32)
            remote = current[row_index]
            remote = jnp.where(live_slots[owner_rank][:, :, None, None], remote, 0.0)
            source_table = jnp.concatenate([own_rows, remote.reshape(2 * REACH * CAP, LEV, NODES * TRACERS)], axis=0)
            dep_block = lax.dynamic_slice_in_dim(departure, owner_rank * ELEMS, ELEMS, 0)
            weight_block = lax.dynamic_slice_in_dim(weights[substep], owner_rank * ELEMS, ELEMS, 0)
            return interpolate(source_table, dep_block, weight_block)

        current = lax.map(per_range, jnp.arange(N_SFC, dtype=jnp.int32)).reshape(ELEMS_ALL, LEV, NODES * TRACERS)
    return current
```

```python
import functools

import jax
import jax.numpy as jnp
from jax import lax
from jax.experimental import pallas as pl
from jax.experimental.pallas import tpu as pltpu
from jax.sharding import PartitionSpec as P

NODES = 16
TRACERS = 30
PADDED = 32
MESH = pl.DeviceIdType.MESH
F32 = jnp.float32
BF16 = jnp.bfloat16


def high_part(value):
    return value.astype(BF16).astype(F32)


def transposed_dot(a, b):
    return lax.dot_general(a, b, (((1,), (1,)), ((), ())), preferred_element_type=F32)


def kernel(
    tracers, weights, departure, needs, counts, out,
    table, picks, mats, slot_ids, wish, asked, rows, sent, got,
    wish_send, wish_got, row_send, row_got,
):
    count = lax.axis_size("sfc")
    me = lax.axis_index("sfc")
    substeps, elements, levels, _ = weights.shape
    sides, cap = asked.shape[0], asked.shape[1]
    reach = sides // 2
    offsets = [j - reach if j < reach else j - reach + 1 for j in range(sides)]
    wide = NODES * PADDED
    narrow = NODES * TRACERS
    remote = sides * cap
    half = NODES // 2

    barrier = pltpu.get_barrier_semaphore()
    for o in offsets:
        pl.semaphore_signal(barrier, inc=1, device_id=(lax.rem(me + o + count, count),), device_id_type=MESH)

    for j in range(sides):
        for c in range(cap):
            wish[j, c : c + 1, :] = jnp.full((1, 128), needs[0, j, c], jnp.int32)

    pl.semaphore_wait(barrier, sides)

    wishes = []
    for j, o in enumerate(offsets):
        copy = pltpu.make_async_remote_copy(
            src_ref=wish.at[j], dst_ref=asked.at[j],
            send_sem=wish_send.at[j], recv_sem=wish_got.at[j],
            device_id=(lax.rem(me + o + count, count),), device_id_type=MESH,
        )
        copy.start()
        wishes.append(copy)

    spread_row = lax.broadcasted_iota(jnp.int32, (wide, narrow), 0)
    spread_col = lax.broadcasted_iota(jnp.int32, (wide, narrow), 1)
    node, tracer = spread_row // PADDED, spread_row % PADDED
    spread = jnp.where((tracer < TRACERS) & (spread_col == node * TRACERS + tracer), 1.0, 0.0).astype(BF16)
    same = jnp.where(
        lax.broadcasted_iota(jnp.int32, (wide, wide), 0) == lax.broadcasted_iota(jnp.int32, (wide, wide), 1), 1.0, 0.0
    ).astype(BF16)

    for l in range(levels):
        own = tracers[:, l, :]
        high = high_part(own)
        parts = jnp.concatenate([high, own - high], axis=0).astype(BF16)
        table[l, :, 0 : 2 * elements] = transposed_dot(spread, parts).astype(BF16)

    def send_rows(s, l):
        lane = lax.broadcasted_iota(jnp.int32, (remote, 2 * elements), 1) % elements
        choice = jnp.where(rows_asked[...] == lane, 1.0, 0.0).astype(BF16)
        chosen = transposed_dot(choice, table[l, :, 0 : 2 * elements])
        copies = []
        for j, o in enumerate(offsets):
            sent[s, l, j] = chosen[j * cap : (j + 1) * cap, :]
        for j, o in enumerate(offsets):
            copy = pltpu.make_async_remote_copy(
                src_ref=sent.at[s, l, j], dst_ref=got.at[s, l, j],
                send_sem=row_send.at[s, l, j], recv_sem=row_got.at[s, l, j],
                device_id=(lax.rem(me - o + count, count),), device_id_type=MESH,
            )
            copy.start()
            copies.append(copy)
        return copies

    rows_asked = rows[1]
    for copy in wishes:
        copy.wait_recv()
    for j in range(sides):
        rows_asked[j * cap : (j + 1) * cap, :] = asked[j]
    flying = [[send_rows(0, l) for l in range(levels)], [None] * levels]

    ids = lax.broadcasted_iota(jnp.int32, (2 * elements, 256), 0) % elements
    slot_ids[0 : 2 * elements, :] = ids
    slot_ids[2 * elements :, :] = jnp.full((256 - 2 * elements, 256), -1, jnp.int32)
    for j in range(sides):
        for c in range(cap):
            slot = j * cap + c
            live = jnp.where(c < counts[0, j], elements + slot, -1)
            line = jnp.full((1, 256), live, jnp.int32)
            for part in range(2):
                at = 2 * elements + part * remote + slot
                slot_ids[at : at + 1, :] = line

    wanted = jnp.transpose(
        jnp.concatenate([departure[...], jnp.zeros((elements, 128 - levels * NODES), jnp.int32)], axis=1).astype(F32)
    ).astype(jnp.int32)
    for l in range(levels):
        first = wanted[l * NODES : l * NODES + half, :]
        second = wanted[l * NODES + half : (l + 1) * NODES, :]
        both = jnp.concatenate([first, second], axis=1)
        for q in range(half // 2):
            target = jnp.concatenate([both[2 * q : 2 * q + 1, :], both[2 * q + 1 : 2 * q + 2, :]], axis=1)
            picks[l, q] = jnp.where(slot_ids[...] == target, 1.0, 0.0).astype(BF16)
        for s in range(substeps):
            matrix = weights[s, :, l, :]
            mats[s, l] = jnp.transpose(jnp.concatenate([matrix[:, : half * NODES], matrix[:, half * NODES :]], axis=0))

    lane = lax.broadcasted_iota(jnp.int32, (PADDED, 2 * elements), 1)
    left = lane < elements

    for s in range(substeps):
        for l in range(levels):
            for copy in flying[s][l]:
                copy.wait_recv()
            for j in range(sides):
                rows[0][j * cap : (j + 1) * cap, :] = got[s, l, j]
            fetched = rows[0][...]
            high = high_part(fetched)
            low = fetched - high
            parts = jnp.concatenate([high, low, high, low], axis=0).astype(BF16)
            table[l, :, 2 * elements :] = transposed_dot(same, parts).astype(BF16)

            fresh = []
            for q in range(half // 2):
                gathered = jnp.dot(table[l], picks[l, q], preferred_element_type=F32)
                for side in range(2):
                    c = 2 * q + side
                    value = lowest = highest = None
                    for k in range(NODES):
                        item = gathered[k * PADDED : (k + 1) * PADDED, side * 128 : (side + 1) * 128]
                        term = mats[s, l, c * NODES + k : c * NODES + k + 1, :] * item
                        value = term if k == 0 else value + term
                        lowest = item if k == 0 else jnp.minimum(lowest, item)
                        highest = item if k == 0 else jnp.maximum(highest, item)
                    value = jnp.clip(value, lowest, highest)
                    other = pltpu.roll(value, elements, 1)
                    value_high, other_high = high_part(value), high_part(other)
                    fresh.append((c, jnp.where(left, value_high, other - other_high).astype(BF16)))
                    fresh.append((c + half, jnp.where(left, other_high, value - value_high).astype(BF16)))
            for t, block in fresh:
                table[l, t * PADDED : (t + 1) * PADDED, 0 : 2 * elements] = block
            if s + 1 < substeps:
                flying[s + 1][l] = send_rows(s + 1, l)
            else:
                packed = lax.dot_general(
                    table[l, :, 0 : 2 * elements], spread, (((0,), (0,)), ((), ())), preferred_element_type=F32
                )
                out[l] = packed[:elements, :] + packed[elements:, :]

    for copy in wishes:
        copy.wait_send()
    for per_level in flying:
        for copies in per_level:
            for copy in copies:
                copy.wait_send()


def on_device(tracers, weights, departure, needs, counts):
    substeps, elements, levels, _ = weights.shape
    sides, cap = needs.shape[1:]
    wide = NODES * PADDED
    vmem = pl.BlockSpec(memory_space=pltpu.VMEM)
    smem = pl.BlockSpec(memory_space=pltpu.SMEM)
    result = pl.pallas_call(
        kernel,
        out_shape=jax.ShapeDtypeStruct((levels, elements, NODES * TRACERS), F32),
        in_specs=[vmem, vmem, vmem, smem, smem],
        out_specs=vmem,
        scratch_shapes=[
            pltpu.VMEM((levels, wide, 256), BF16),
            pltpu.VMEM((levels, NODES * elements // 256, 256, 256), BF16),
            pltpu.VMEM((substeps, levels, NODES * NODES // 2, 2 * elements), F32),
            pltpu.VMEM((256, 256), jnp.int32),
            pltpu.VMEM((sides, cap, 128), jnp.int32),
            pltpu.VMEM((sides, cap, 128), jnp.int32),
            [pltpu.VMEM((sides * cap, wide), F32), pltpu.VMEM((sides * cap, 128), jnp.int32)],
            pltpu.VMEM((substeps, levels, sides, cap, wide), F32),
            pltpu.VMEM((substeps, levels, sides, cap, wide), F32),
            pltpu.SemaphoreType.DMA((sides,)),
            pltpu.SemaphoreType.DMA((sides,)),
            pltpu.SemaphoreType.DMA((substeps, levels, sides)),
            pltpu.SemaphoreType.DMA((substeps, levels, sides)),
        ],
        compiler_params=pltpu.CompilerParams(collective_id=0, has_side_effects=True, vmem_limit_bytes=60 << 20),
    )(tracers, weights, departure, needs, counts)
    return jnp.transpose(result, (1, 0, 2))


def solution(mesh):
    return jax.shard_map(
        on_device,
        mesh=mesh,
        in_specs=(
            P("sfc", None, None),
            P(None, "sfc", None, None),
            P("sfc", None),
            P("sfc", None, None),
            P("sfc", None),
        ),
        out_specs=P("sfc", None, None),
        check_vma=False,
    )
```

```python
import functools

import jax
import jax.numpy as jnp
from jax import lax
from jax.experimental import pallas as pl
from jax.experimental.pallas import tpu as pltpu
from jax.sharding import PartitionSpec as P

NODES = 16
TRACERS = 30
PADDED = 32
MESH = pl.DeviceIdType.MESH
F32 = jnp.float32
BF16 = jnp.bfloat16


def high_part(value):
    return value.astype(BF16).astype(F32)


def transposed_dot(a, b):
    return lax.dot_general(a, b, (((1,), (1,)), ((), ())), preferred_element_type=F32)


def kernel(
    tracers, weights, departure, needs, counts, out,
    table, picks, mats, slot_ids, wish, asked, rows, sent, got,
    wish_send, wish_got, row_send, row_got,
):
    count = lax.axis_size("sfc")
    me = lax.axis_index("sfc")
    substeps, levels, elements, _ = weights.shape
    sides, cap = asked.shape[0], asked.shape[1]
    reach = sides // 2
    offsets = [j - reach if j < reach else j - reach + 1 for j in range(sides)]
    wide = NODES * PADDED
    narrow = NODES * TRACERS
    remote = sides * cap
    half = NODES // 2

    barrier = pltpu.get_barrier_semaphore()
    for o in offsets:
        pl.semaphore_signal(barrier, inc=1, device_id=(lax.rem(me + o + count, count),), device_id_type=MESH)

    for j in range(sides):
        for c in range(cap):
            wish[j, c : c + 1, :] = jnp.full((1, 128), needs[0, c, j], jnp.int32)

    pl.semaphore_wait(barrier, sides)

    wishes = []
    for j, o in enumerate(offsets):
        copy = pltpu.make_async_remote_copy(
            src_ref=wish.at[j], dst_ref=asked.at[j],
            send_sem=wish_send.at[j], recv_sem=wish_got.at[j],
            device_id=(lax.rem(me + o + count, count),), device_id_type=MESH,
        )
        copy.start()
        wishes.append(copy)

    spread_row = lax.broadcasted_iota(jnp.int32, (wide, narrow), 0)
    spread_col = lax.broadcasted_iota(jnp.int32, (wide, narrow), 1)
    node, tracer = spread_row // PADDED, spread_row % PADDED
    spread = jnp.where((tracer < TRACERS) & (spread_col == node * TRACERS + tracer), 1.0, 0.0).astype(BF16)
    same = jnp.where(
        lax.broadcasted_iota(jnp.int32, (wide, wide), 0) == lax.broadcasted_iota(jnp.int32, (wide, wide), 1), 1.0, 0.0
    ).astype(BF16)

    for l in range(levels):
        own = tracers[l]
        high = high_part(own)
        parts = jnp.concatenate([high, own - high], axis=0).astype(BF16)
        table[l, :, 0 : 2 * elements] = transposed_dot(spread, parts).astype(BF16)

    def send_rows(s, l):
        lane = lax.broadcasted_iota(jnp.int32, (remote, 2 * elements), 1) % elements
        choice = jnp.where(rows_asked[...] == lane, 1.0, 0.0).astype(BF16)
        chosen = transposed_dot(choice, table[l, :, 0 : 2 * elements])
        copies = []
        for j, o in enumerate(offsets):
            sent[s, l, j] = chosen[j * cap : (j + 1) * cap, :]
        for j, o in enumerate(offsets):
            copy = pltpu.make_async_remote_copy(
                src_ref=sent.at[s, l, j], dst_ref=got.at[s, l, j],
                send_sem=row_send.at[s, l, j], recv_sem=row_got.at[s, l, j],
                device_id=(lax.rem(me - o + count, count),), device_id_type=MESH,
            )
            copy.start()
            copies.append(copy)
        return copies

    rows_asked = rows[1]
    for copy in wishes:
        copy.wait_recv()
    for j in range(sides):
        rows_asked[j * cap : (j + 1) * cap, :] = asked[j]
    flying = [[send_rows(0, l) for l in range(levels)], [None] * levels]

    ids = lax.broadcasted_iota(jnp.int32, (2 * elements, 256), 0) % elements
    slot_ids[0 : 2 * elements, :] = ids
    slot_ids[2 * elements :, :] = jnp.full((256 - 2 * elements, 256), -1, jnp.int32)
    for j in range(sides):
        for c in range(cap):
            slot = j * cap + c
            live = jnp.where(c < counts[0, j], elements + slot, -1)
            line = jnp.full((1, 256), live, jnp.int32)
            for part in range(2):
                at = 2 * elements + part * remote + slot
                slot_ids[at : at + 1, :] = line

    for l in range(levels):
        first = departure[l * NODES : l * NODES + half, :]
        second = departure[l * NODES + half : (l + 1) * NODES, :]
        both = jnp.concatenate([first, second], axis=1)
        for q in range(half // 2):
            target = jnp.concatenate([both[2 * q : 2 * q + 1, :], both[2 * q + 1 : 2 * q + 2, :]], axis=1)
            picks[l, q] = jnp.where(slot_ids[...] == target, 1.0, 0.0).astype(BF16)
        for s in range(substeps):
            matrix = weights[s, l]
            mats[s, l] = jnp.transpose(jnp.concatenate([matrix[:, : half * NODES], matrix[:, half * NODES :]], axis=0))

    lane = lax.broadcasted_iota(jnp.int32, (PADDED, 2 * elements), 1)
    left = lane < elements

    for s in range(substeps):
        for l in range(levels):
            for copy in flying[s][l]:
                copy.wait_recv()
            for j in range(sides):
                rows[0][j * cap : (j + 1) * cap, :] = got[s, l, j]
            fetched = rows[0][...]
            high = high_part(fetched)
            low = fetched - high
            parts = jnp.concatenate([high, low, high, low], axis=0).astype(BF16)
            table[l, :, 2 * elements :] = transposed_dot(same, parts).astype(BF16)

            fresh = []
            for q in range(half // 2):
                gathered = jnp.dot(table[l], picks[l, q], preferred_element_type=F32)
                for side in range(2):
                    c = 2 * q + side
                    value = lowest = highest = None
                    for k in range(NODES):
                        item = gathered[k * PADDED : (k + 1) * PADDED, side * 128 : (side + 1) * 128]
                        term = mats[s, l, c * NODES + k : c * NODES + k + 1, :] * item
                        value = term if k == 0 else value + term
                        lowest = item if k == 0 else jnp.minimum(lowest, item)
                        highest = item if k == 0 else jnp.maximum(highest, item)
                    value = jnp.clip(value, lowest, highest)
                    other = pltpu.roll(value, elements, 1)
                    value_high, other_high = high_part(value), high_part(other)
                    fresh.append((c, jnp.where(left, value_high, other - other_high).astype(BF16)))
                    fresh.append((c + half, jnp.where(left, other_high, value - value_high).astype(BF16)))
            for t, block in fresh:
                table[l, t * PADDED : (t + 1) * PADDED, 0 : 2 * elements] = block
            if s + 1 < substeps:
                flying[s + 1][l] = send_rows(s + 1, l)
            else:
                packed = lax.dot_general(
                    table[l, :, 0 : 2 * elements], spread, (((0,), (0,)), ((), ())), preferred_element_type=F32
                )
                out[l] = packed[:elements, :] + packed[elements:, :]

    for copy in wishes:
        copy.wait_send()
    for per_level in flying:
        for copies in per_level:
            for copy in copies:
                copy.wait_send()


def on_device(tracers, weights, departure, needs, counts):
    substeps, elements, levels, _ = weights.shape
    sides, cap = needs.shape[1:]
    wide = NODES * PADDED
    vmem = pl.BlockSpec(memory_space=pltpu.VMEM)
    smem = pl.BlockSpec(memory_space=pltpu.SMEM)
    result = pl.pallas_call(
        kernel,
        out_shape=jax.ShapeDtypeStruct((levels, elements, NODES * TRACERS), F32),
        in_specs=[vmem, vmem, vmem, smem, smem],
        out_specs=vmem,
        scratch_shapes=[
            pltpu.VMEM((levels, wide, 256), BF16),
            pltpu.VMEM((levels, NODES * elements // 256, 256, 256), BF16),
            pltpu.VMEM((substeps, levels, NODES * NODES // 2, 2 * elements), F32),
            pltpu.VMEM((256, 256), jnp.int32),
            pltpu.VMEM((sides, cap, 128), jnp.int32),
            pltpu.VMEM((sides, cap, 128), jnp.int32),
            [pltpu.VMEM((sides * cap, wide), F32), pltpu.VMEM((sides * cap, 128), jnp.int32)],
            pltpu.VMEM((substeps, levels, sides, cap, wide), F32),
            pltpu.VMEM((substeps, levels, sides, cap, wide), F32),
            pltpu.SemaphoreType.DMA((sides,)),
            pltpu.SemaphoreType.DMA((sides,)),
            pltpu.SemaphoreType.DMA((substeps, levels, sides)),
            pltpu.SemaphoreType.DMA((substeps, levels, sides)),
        ],
        compiler_params=pltpu.CompilerParams(collective_id=0, has_side_effects=True, vmem_limit_bytes=60 << 20),
    )(
        jnp.transpose(tracers, (1, 0, 2)),
        jnp.transpose(weights, (0, 2, 1, 3)),
        jnp.transpose(departure),
        jnp.transpose(needs, (0, 2, 1)),
        counts,
    )
    return jnp.transpose(result, (1, 0, 2))


def solution(mesh):
    return jax.shard_map(
        on_device,
        mesh=mesh,
        in_specs=(
            P("sfc", None, None),
            P(None, "sfc", None, None),
            P("sfc", None),
            P("sfc", None, None),
            P("sfc", None),
        ),
        out_specs=P("sfc", None, None),
        check_vma=False,
    )
```

```python
import functools

import jax
import jax.numpy as jnp
from jax import lax
from jax.experimental import pallas as pl
from jax.experimental.pallas import tpu as pltpu
from jax.sharding import PartitionSpec as P

NODES = 16
TRACERS = 30
PADDED = 32
MESH = pl.DeviceIdType.MESH
F32 = jnp.float32
BF16 = jnp.bfloat16


def high_part(value):
    return value.astype(BF16).astype(F32)


def transposed_dot(a, b):
    return lax.dot_general(a, b, (((1,), (1,)), ((), ())), preferred_element_type=F32)


def kernel(
    tracers_far, weights_far, departure_far, needs, counts, out_far,
    tracers, weights, departure, out, table, picks, mats, slot_ids, wish, asked, rows, rows_asked, sent, got,
    spread, same, wish_send, wish_got, row_send, row_got, loaded, stored,
):
    count = lax.axis_size("sfc")
    me = lax.axis_index("sfc")
    substeps, levels, elements, _ = weights.shape
    sides, cap = asked.shape[0], asked.shape[1]
    reach = sides // 2
    offsets = [j - reach if j < reach else j - reach + 1 for j in range(sides)]
    wide = NODES * PADDED
    narrow = NODES * TRACERS
    remote = sides * cap
    half = NODES // 2
    own_lanes = 2 * elements

    def device(offset):
        return (lax.rem(me + offset + count, count),)

    barrier = pltpu.get_barrier_semaphore()
    for o in offsets:
        pl.semaphore_signal(barrier, inc=1, device_id=device(o), device_id_type=MESH)

    loads = [
        pltpu.make_async_copy(far, near, loaded.at[i])
        for i, (far, near) in enumerate(((tracers_far, tracers), (departure_far, departure), (weights_far, weights)))
    ]
    for load in loads:
        load.start()

    for j in range(sides):
        for c in range(cap):
            wish[j, c : c + 1, :] = jnp.full((1, 128), needs[0, c, j], jnp.int32)

    pl.semaphore_wait(barrier, sides)

    wishes = []
    for j, o in enumerate(offsets):
        copy = pltpu.make_async_remote_copy(
            src_ref=wish.at[j], dst_ref=asked.at[j],
            send_sem=wish_send.at[j], recv_sem=wish_got.at[j],
            device_id=device(o), device_id_type=MESH,
        )
        copy.start()
        wishes.append(copy)

    def row_copy(s, l, j):
        return pltpu.make_async_remote_copy(
            src_ref=sent.at[s, l, j], dst_ref=got.at[s, l, j],
            send_sem=row_send.at[s, l, j], recv_sem=row_got.at[s, l, j],
            device_id=device(-offsets[j]), device_id_type=MESH,
        )

    def build_spread(k, _):
        tracer = lax.broadcasted_iota(jnp.int32, (PADDED, narrow), 0)
        column = lax.broadcasted_iota(jnp.int32, (PADDED, narrow), 1) - k * TRACERS
        column = jnp.where(tracer < TRACERS, column, -1)
        spread[pl.ds(pl.multiple_of(k * PADDED, PADDED), PADDED), :] = jnp.where(column == tracer, 1.0, 0.0).astype(BF16)
        return 0

    lax.fori_loop(0, NODES, build_spread, 0)
    same[...] = jnp.where(
        lax.broadcasted_iota(jnp.int32, (128, 128), 0) == lax.broadcasted_iota(jnp.int32, (128, 128), 1), 1.0, 0.0
    ).astype(BF16)

    loads[0].wait()

    def build_table(l, _):
        own = tracers[l]
        high = high_part(own)
        parts = jnp.concatenate([high, own - high], axis=0).astype(BF16)
        table[0, l, :, 0:own_lanes] = transposed_dot(spread[...], parts).astype(BF16)
        return 0

    for l in range(levels):
        build_table(l, 0)

    def send_rows(s, l):
        lane = lax.broadcasted_iota(jnp.int32, (remote, own_lanes), 1) % elements
        choice = jnp.where(rows_asked[...] == lane, 1.0, 0.0).astype(BF16)
        chosen = transposed_dot(choice, table[s, l, :, 0:own_lanes])
        for j in range(sides):
            sent[s, l, j] = chosen[j * cap : (j + 1) * cap, :]
        for j in range(sides):
            row_copy(s, l, j).start()

    for copy in wishes:
        copy.wait_recv()
    for j in range(sides):
        rows_asked[j * cap : (j + 1) * cap, :] = asked[j]

    def first_rows(l, _):
        send_rows(0, l)
        return 0

    for l in range(levels):
        first_rows(l, 0)

    slot_ids[0:own_lanes, :] = lax.broadcasted_iota(jnp.int32, (own_lanes, 256), 0) % elements
    slot_ids[own_lanes:, :] = jnp.full((256 - own_lanes, 256), -1, jnp.int32)
    for j in range(sides):
        for c in range(cap):
            slot = j * cap + c
            live = jnp.where(c < counts[0, j], elements + slot, -1)
            line = jnp.full((1, 256), live, jnp.int32)
            for part in range(2):
                at = own_lanes + part * remote + slot
                slot_ids[at : at + 1, :] = line

    loads[1].wait()
    loads[2].wait()

    def build_picks(l, _):
        base = l * NODES
        first = departure[pl.ds(base, half), :]
        second = departure[pl.ds(base + half, half), :]
        both = jnp.concatenate([first, second], axis=1)
        for q in range(half // 2):
            target = jnp.concatenate([both[2 * q : 2 * q + 1, :], both[2 * q + 1 : 2 * q + 2, :]], axis=1)
            picks[l, q] = jnp.where(slot_ids[...] == target, 1.0, 0.0).astype(BF16)
        for s in range(substeps):
            matrix = weights[s, l]
            mats[s, l] = jnp.transpose(jnp.concatenate([matrix[:, : half * NODES], matrix[:, half * NODES :]], axis=0))
        return 0

    for l in range(levels):
        build_picks(l, 0)

    left = lax.broadcasted_iota(jnp.int32, (PADDED, own_lanes), 1) < elements

    def one_level(turn, _):
        s, l = turn // levels, turn % levels
        for j in range(sides):
            row_copy(s, l, j).wait_recv()
        for j in range(sides):
            rows[j * cap : (j + 1) * cap, :] = got[s, l, j]
        fetched = rows[...]
        high = high_part(fetched)
        low = fetched - high
        parts = jnp.concatenate([high, low, high, low], axis=0).astype(BF16)
        for at in range(0, wide, 128):
            table[s, l, at : at + 128, own_lanes:] = transposed_dot(same[...], parts[:, at : at + 128]).astype(BF16)

        def one_pair(q, _):
            gathered = jnp.dot(table[s, l], picks[l, q], preferred_element_type=F32)
            for side in range(2):
                c = 2 * q + side
                matrix = mats[s, l, pl.ds(c * NODES, NODES), :]
                value = lowest = highest = None
                for k in range(NODES):
                    item = gathered[k * PADDED : (k + 1) * PADDED, side * 128 : (side + 1) * 128]
                    term = matrix[k : k + 1, :] * item
                    value = term if k == 0 else value + term
                    lowest = item if k == 0 else jnp.minimum(lowest, item)
                    highest = item if k == 0 else jnp.maximum(highest, item)
                value = jnp.clip(value, lowest, highest)
                other = pltpu.roll(value, elements, 1)
                value_high, other_high = high_part(value), high_part(other)
                near = c * PADDED
                past = (c + half) * PADDED
                table[s + 1, l, pl.ds(near, PADDED), 0:own_lanes] = jnp.where(left, value_high, other - other_high).astype(BF16)
                table[s + 1, l, pl.ds(past, PADDED), 0:own_lanes] = jnp.where(left, other_high, value - value_high).astype(BF16)
            return 0

        for q in range(half // 2):
            one_pair(q, 0)

        if s + 1 < substeps:
            send_rows(s + 1, l)

        else:
            packed = lax.dot_general(
                table[s + 1, l, :, 0:own_lanes], spread[...], (((0,), (0,)), ((), ())), preferred_element_type=F32
            )
            out[l] = packed[:elements, :] + packed[elements:, :]
            pltpu.make_async_copy(out.at[l], out_far.at[l], stored.at[l]).start()

        return 0

    for turn in range(substeps * levels):
        one_level(turn, 0)

    for copy in wishes:
        copy.wait_send()
    for s in range(substeps):
        for l in range(levels):
            for j in range(sides):
                row_copy(s, l, j).wait_send()
    for l in range(levels):
        pltpu.make_async_copy(out.at[l], out_far.at[l], stored.at[l]).wait()


def on_device(tracers, weights, departure, needs, counts):
    substeps, elements, levels, _ = weights.shape
    sides, cap = needs.shape[1:]
    wide = NODES * PADDED
    far = pl.BlockSpec(memory_space=pl.ANY)
    smem = pl.BlockSpec(memory_space=pltpu.SMEM)
    result = pl.pallas_call(
        kernel,
        out_shape=jax.ShapeDtypeStruct((levels, elements, NODES * TRACERS), F32),
        in_specs=[far, far, far, smem, smem],
        out_specs=far,
        scratch_shapes=[
            pltpu.VMEM((levels, elements, NODES * TRACERS), F32),
            pltpu.VMEM((substeps, levels, elements, NODES * NODES), F32),
            pltpu.VMEM((levels * NODES, elements), jnp.int32),
            pltpu.VMEM((levels, elements, NODES * TRACERS), F32),
            pltpu.VMEM((substeps + 1, levels, wide, 256), BF16),
            pltpu.VMEM((levels, NODES * elements // 256, 256, 256), BF16),
            pltpu.VMEM((substeps, levels, NODES * NODES // 2, 2 * elements), F32),
            pltpu.VMEM((256, 256), jnp.int32),
            pltpu.VMEM((sides, cap, 128), jnp.int32),
            pltpu.VMEM((sides, cap, 128), jnp.int32),
            pltpu.VMEM((sides * cap, wide), F32),
            pltpu.VMEM((sides * cap, 128), jnp.int32),
            pltpu.VMEM((substeps, levels, sides, cap, wide), F32),
            pltpu.VMEM((substeps, levels, sides, cap, wide), F32),
            pltpu.VMEM((wide, NODES * TRACERS), BF16),
            pltpu.VMEM((128, 128), BF16),
            pltpu.SemaphoreType.DMA((sides,)),
            pltpu.SemaphoreType.DMA((sides,)),
            pltpu.SemaphoreType.DMA((substeps, levels, sides)),
            pltpu.SemaphoreType.DMA((substeps, levels, sides)),
            pltpu.SemaphoreType.DMA((3,)),
            pltpu.SemaphoreType.DMA((levels,)),
        ],
        compiler_params=pltpu.CompilerParams(collective_id=0, has_side_effects=True, vmem_limit_bytes=60 << 20),
    )(
        jnp.transpose(tracers, (1, 0, 2)),
        jnp.transpose(weights, (0, 2, 1, 3)),
        jnp.transpose(departure),
        jnp.transpose(needs, (0, 2, 1)),
        counts,
    )
    return jnp.transpose(result, (1, 0, 2))


def solution(mesh):
    return jax.shard_map(
        on_device,
        mesh=mesh,
        in_specs=(
            P("sfc", None, None),
            P(None, "sfc", None, None),
            P("sfc", None),
            P("sfc", None, None),
            P("sfc", None),
        ),
        out_specs=P("sfc", None, None),
        check_vma=False,
    )
```
